8 devices in a mesh: dp: 2 (over y, z), tp: 4 (over x, core).
Axes of the slice: x: 2, y: 2, z: 1, core: 2. Of those that a mesh axis runs over, the one named last changes fastest.
Arguments:
- x: bfloat16 [4096, 4096], P('dp'), parts along dimension 0
- gain: bfloat16 [4096], replicated
- wq: bfloat16 [4096, 6144], P(None, 'tp')
- wk: bfloat16 [4096, 1024], P(None, 'tp')
- wv: bfloat16 [4096, 1024], P(None, 'tp')
- wo: bfloat16 [6144, 4096], P('tp')
Outputs:
- output: bfloat16 [4096, 4096], P('dp'), parts along dimension 0
There are 2 independent parts. The reference program is written for one: setup_inputs(seed, part) draws one part's arguments, and reference() takes and returns one part's arrays. A program takes and returns all parts, laid end to end along the dimension named above; an argument that names none is the same for every part.
All inputs are finite; a program needn't handle non-finite values.
Results may differ from the reference program's by a relative error of at most 0.012.
Values are sent between devices in bfloat16 or wider.
A program may use at most 2 GiB of HBM per device.

```python
import jax
import jax.numpy as jnp
from jax import lax

ROWS = 2048
D = 4096
HEADS = 48
KV_HEADS = 8
HEAD = 128
THETA = 10000


def setup_inputs(seed: int = 0, part: int = 0) -> dict:
    kx, kn, kq, kk, kv, ko = jax.random.split(jax.random.key(seed), 6)

    def weights(key, rows, columns):
        return jax.random.normal(key, (rows, columns), jnp.float32) * rows**-0.5

    drawn = {
        "x": jax.random.normal(jax.random.fold_in(kx, part), (ROWS, D), jnp.float32),
        "gain": 1 + 0.1 * jax.random.normal(kn, (D,), jnp.float32),
        "wq": 2 * weights(kq, D, HEADS * HEAD),
        "wk": 2 * weights(kk, D, KV_HEADS * HEAD),
        "wv": 4 * weights(kv, D, KV_HEADS * HEAD),
        "wo": weights(ko, HEADS * HEAD, D),
    }
    return {k: v.astype(jnp.bfloat16) for k, v in drawn.items()}


def normed(x, gain):
    wide = x.astype(jnp.float32)
    scale = lax.rsqrt(jnp.mean(wide * wide, -1, keepdims=True) + 1e-6)
    return (wide * scale * gain.astype(jnp.float32)).astype(jnp.bfloat16)


def turned(t, place, theta):
    half = t.shape[-1] // 2
    angle = place.astype(jnp.float32)[:, None] * theta ** (-jnp.arange(half, dtype=jnp.float32) / half)
    cos, sin = jnp.cos(angle)[:, None], jnp.sin(angle)[:, None]
    a, b = t[..., :half].astype(jnp.float32), t[..., half:].astype(jnp.float32)
    return jnp.concatenate([a * cos - b * sin, b * cos + a * sin], -1).astype(jnp.bfloat16)


def matmul(a, w):
    return jnp.dot(a, w, preferred_element_type=jnp.float32).astype(jnp.bfloat16)


def einsum(form, a, b):
    return jnp.einsum(form, a.astype(jnp.float32), b.astype(jnp.float32))


def attention(q, k, v):
    scores = einsum("tgsd,ugd->gstu", q, k) * q.shape[-1] ** -0.5
    token = jnp.arange(q.shape[0])
    scores = jnp.where(token[:, None] >= token, scores, -jnp.inf)
    weights = jax.nn.softmax(scores, -1).astype(jnp.bfloat16)
    return einsum("gstu,ugd->tgsd", weights, v).astype(jnp.bfloat16)


def reference(x, gain, wq, wk, wv, wo):
    a, place = normed(x, gain), jnp.arange(ROWS)
    q = turned(matmul(a, wq).reshape(ROWS, HEADS, HEAD), place, THETA).reshape(ROWS, KV_HEADS, -1, HEAD)
    k = turned(matmul(a, wk).reshape(ROWS, KV_HEADS, HEAD), place, THETA)
    v = matmul(a, wv).reshape(ROWS, KV_HEADS, HEAD)
    seen = attention(q, k, v).reshape(ROWS, HEADS * HEAD)
    return (x.astype(jnp.float32) + jnp.dot(seen, wo, preferred_element_type=jnp.float32)).astype(jnp.bfloat16)
```

```python
import functools

import jax
import jax.numpy as jnp
import numpy as np
from jax import lax
from jax.experimental import pallas as pl
from jax.experimental.pallas import tpu as pltpu
from jax.sharding import PartitionSpec as P

HEAD = 128
THETA = 10000
LOG2E = 1.4426950408889634
HIDDEN = -2e30
ROWS = 128
KEYS = 256
LAG = 3
WIDE = 512
MESH = pl.DeviceIdType.MESH
VMEM = 67_043_328


def _dot(a, b, ca, cb):
    return lax.dot_general(a, b, (((ca,), (cb,)), ((), ())), preferred_element_type=jnp.float32)


def _tables(rows, chunks):
    half = HEAD // 2
    rate = THETA ** (-np.arange(half, dtype=np.float64) / half)
    rate = np.concatenate([rate, rate])
    a = np.arange(rows)[:, None] * rate
    b = (np.arange(chunks) * rows)[:, None] * rate
    return [t.astype(np.float32) for t in (np.cos(a), np.sin(a), np.cos(b), np.sin(b))]


def _layer(x, gain, cos_a, sin_a, cos_b, sin_b, wq, wk, wv, wo, out,
           wq_s, wkv_s, wo_far, wo_near, x_s, res_s, a_s, q_s, k_s, v_s, top_s, mix_s, seen_s, near_s, far_s, got_s, sum_s, peer_s,
           w_sem, x_sem, res_sem, far_send, far_recv, free, sum_send, sum_recv, put_sem, give_send, give_recv):
    t = lax.axis_index("tp")
    core = lax.rem(t, 2)
    sibling = {"tp": t + 1 - 2 * core}
    partner = {"tp": lax.rem(t + 2, 4)}
    total_rows, d = x.shape
    chunks = total_rows // ROWS
    half = d // 2
    kv = k_s.shape[0]
    cols = q_s.shape[1]
    group = cols // ROWS
    near_cols = pl.ds(pl.multiple_of(core * half, half), half)
    far_cols = lambda at: pl.ds(pl.multiple_of((1 - core) * half + at, WIDE), WIDE)
    own_cols = lambda at: pl.ds(pl.multiple_of(core * half + at, WIDE), WIDE)
    nq = wq.shape[1] // WIDE
    nk = wk.shape[1]
    no = half // WIDE

    def rows_of(c):
        return pl.ds(pl.multiple_of(c * ROWS, ROWS), ROWS)

    weights = [(wk, wkv_s.at[:, pl.ds(0, nk)]), (wv, wkv_s.at[:, pl.ds(nk, nk)])]
    weights += [(wq.at[:, pl.ds(n * WIDE, WIDE)], wq_s.at[:, pl.ds(n * WIDE, WIDE)]) for n in range(nq)]
    weights += [(wo.at[:, far_cols(n * WIDE)], wo_far.at[:, pl.ds(n * WIDE, WIDE)]) for n in range(no)]
    weights += [(wo.at[:, own_cols(n * WIDE)], wo_near.at[:, pl.ds(n * WIDE, WIDE)]) for n in range(no)]
    weights = [pltpu.make_async_copy(src, dst, w_sem.at[n]) for n, (src, dst) in enumerate(weights)]

    def x_copy(c):
        return pltpu.make_async_copy(x.at[rows_of(c), :], x_s.at[lax.rem(c, 2)], x_sem.at[lax.rem(c, 2)])

    def res_copy(f):
        return pltpu.make_async_copy(x.at[rows_of(f), near_cols], res_s.at[lax.rem(f, 2)], res_sem.at[lax.rem(f, 2)])

    def far_copy():
        return pltpu.make_async_remote_copy(src_ref=far_s, dst_ref=got_s, send_sem=far_send, recv_sem=far_recv, device_id=sibling, device_id_type=MESH)

    def sum_copy(c):
        return pltpu.make_async_remote_copy(src_ref=sum_s.at[c], dst_ref=peer_s.at[c], send_sem=sum_send.at[c], recv_sem=sum_recv.at[c],
                                            device_id=partner, device_id_type=MESH)

    def put_copy(f):
        return pltpu.make_async_copy(sum_s.at[f], out.at[rows_of(f), near_cols], put_sem.at[f])

    def give_copy(f):
        return pltpu.make_async_remote_copy(src_ref=sum_s.at[f], dst_ref=out.at[rows_of(f), near_cols], send_sem=give_send.at[f],
                                            recv_sem=give_recv.at[f], device_id=sibling, device_id_type=MESH)

    x_copy(0).start()
    for w in weights:
        w.start()
    barrier = pltpu.get_barrier_semaphore()
    for other in (sibling, partner):
        pl.semaphore_signal(barrier, inc=1, device_id=other, device_id_type=MESH)
    k_s[...] = jnp.zeros_like(k_s)
    v_s[...] = jnp.zeros_like(v_s)
    for i in range(kv):
        v_s[i, HEAD:, :] = jnp.ones((v_s.shape[1] - HEAD, v_s.shape[2]), v_s.dtype)
    pl.semaphore_wait(barrier, 2)

    def finish(f):
        res_copy(f).wait()
        sum_copy(f).wait()
        slot = lax.rem(f, 2)

        @pl.loop(0, ROWS // 16)
        def _(r):
            at = pl.ds(pl.multiple_of(r * 16, 16), 16)
            term = sum_s[f, at, :].astype(jnp.float32) + peer_s[f, at, :].astype(jnp.float32)
            sum_s[f, at, :] = (res_s[slot, at, :].astype(jnp.float32) + term).astype(jnp.bfloat16)

        put_copy(f).start()
        give_copy(f).start()

    e = HEAD**-0.5 * LOG2E
    strip = cols // 2
    pieces = [(i, at) for i in range(kv) for at in range(0, cols, strip)]

    def first_use(c, n):
        @pl.when(c == 0)
        def _():
            weights[n].wait()

    def attend(c):
        blocks = lax.div(c * ROWS, KEYS)

        def block(j, diagonal):
            here = pl.ds(pl.multiple_of(j * KEYS, KEYS), KEYS)
            scores = [_dot(k_s[i, here, :], q_s[i, at : at + strip, :], 1, 1) for i, at in pieces]
            if diagonal:
                key = lax.broadcasted_iota(jnp.int32, (KEYS, strip), 0)
                query = lax.rem(lax.broadcasted_iota(jnp.int32, (KEYS, strip), 1), ROWS)
                ok = query - key >= j * KEYS - c * ROWS
            probs, keeps = [], []
            for (i, at), s in zip(pieces, scores):
                span = pl.ds(at, strip)
                if diagonal:
                    s = jnp.where(ok, s, HIDDEN)
                    top = s.max(axis=0, keepdims=True)
                else:
                    old = top_s[i : i + 1, span]
                    top = jnp.maximum(old, s.max(axis=0, keepdims=True))
                    keeps.append(jnp.exp2((old - top) * e))
                top_s[i : i + 1, span] = top
                probs.append(jnp.exp2((s - top) * e).astype(jnp.bfloat16))
            for n, ((i, at), p) in enumerate(zip(pieces, probs)):
                span = pl.ds(at, strip)
                new = _dot(v_s[i, :, here], p, 1, 0)
                mix_s[i, :, span] = new if diagonal else mix_s[i, :, span] * keeps[n] + new

        block(blocks, True)
        lax.fori_loop(0, blocks, lambda j, _: block(j, False), None)
        for i in range(kv):
            done = mix_s[i, :HEAD, :] * (1 / mix_s[i, HEAD : HEAD + 1, :])
            done = done.T.astype(jnp.bfloat16)
            for n in range(group):
                h = i * group + n
                seen_s[:, h * HEAD : (h + 1) * HEAD] = done[n * ROWS : (n + 1) * ROWS, :]

    @pl.loop(0, chunks)
    def _(c):
        slot = lax.rem(c, 2)
        x_copy(c).wait()

        @pl.when(c + 1 < chunks)
        def _():
            x_copy(c + 1).start()

        @pl.when(c >= LAG)
        def _():
            res_copy(c - LAG).start()

        @pl.loop(0, ROWS // 16)
        def _(r):
            at = pl.ds(pl.multiple_of(r * 16, 16), 16)
            wide = x_s[slot, at, :].astype(jnp.float32)
            scale = lax.rsqrt(jnp.mean(wide * wide, -1, keepdims=True) + 1e-6)
            a_s[at, :] = (wide * scale * gain[...].astype(jnp.float32)).astype(jnp.bfloat16)

        sign = jnp.where(lax.broadcasted_iota(jnp.int32, (ROWS, HEAD), 1) < HEAD // 2, -1.0, 1.0)
        cb, sb = cos_b[pl.ds(c, 1), :], sin_b[pl.ds(c, 1), :]
        cos = cos_a[...] * cb - sin_a[...] * sb
        sin = (sin_a[...] * cb + cos_a[...] * sb) * sign

        def turned(u):
            u = u.astype(jnp.float32)
            return (u * cos + pltpu.roll(u, HEAD // 2, 1) * sin).astype(jnp.bfloat16)

        first_use(c, 0)
        first_use(c, 1)
        both = _dot(a_s[...], wkv_s[...], 1, 0).astype(jnp.bfloat16)
        for i in range(kv):
            k_s[i, rows_of(c), :] = turned(both[:, i * HEAD : (i + 1) * HEAD])
            v_s[i, :HEAD, rows_of(c)] = both[:, nk + i * HEAD : nk + (i + 1) * HEAD].T
        for n in range(nq):
            first_use(c, 2 + n)
            part = _dot(a_s[...], wq_s[:, n * WIDE : (n + 1) * WIDE], 1, 0).astype(jnp.bfloat16)
            for m in range(WIDE // HEAD):
                h = n * (WIDE // HEAD) + m
                q_s[h // group, (h % group) * ROWS : (h % group + 1) * ROWS, :] = turned(part[:, m * HEAD : (m + 1) * HEAD])

        attend(c)

        @pl.when(c >= 1)
        def _():
            pl.semaphore_wait(free, 1)

        for n in range(no):
            first_use(c, 2 + nq + n)
            far_s[:, n * WIDE : (n + 1) * WIDE] = _dot(seen_s[...], wo_far[:, n * WIDE : (n + 1) * WIDE], 1, 0).astype(jnp.bfloat16)
        far_copy().start()
        for n in range(no):
            first_use(c, 2 + nq + no + n)
            near_s[:, n * WIDE : (n + 1) * WIDE] = _dot(seen_s[...], wo_near[:, n * WIDE : (n + 1) * WIDE], 1, 0)

        far_copy().wait()

        @pl.loop(0, ROWS // 16)
        def _(r):
            at = pl.ds(pl.multiple_of(r * 16, 16), 16)
            sum_s[c, at, :] = (near_s[at, :] + got_s[at, :].astype(jnp.float32)).astype(jnp.bfloat16)

        sum_copy(c).start()

        @pl.when(c + 1 < chunks)
        def _():
            pl.semaphore_signal(free, inc=1, device_id=sibling, device_id_type=MESH)

        @pl.when(c >= LAG)
        def _():
            finish(c - LAG)

    @pl.loop(chunks - LAG, chunks)
    def _(f):
        res_copy(f).start()
        finish(f)

    @pl.loop(0, chunks)
    def _(f):
        put_copy(f).wait()
        give_copy(f).wait()


def solution(mesh):
    def step(x, gain, wq, wk, wv, wo):
        rows, d = x.shape
        chunks = rows // ROWS
        kv = wk.shape[1] // HEAD
        heads = wq.shape[1] // HEAD
        cols = heads // kv * ROWS
        half = d // 2
        bf, f32 = jnp.bfloat16, jnp.float32
        n_weights = 2 + wq.shape[1] // WIDE + d // WIDE
        dma = pltpu.SemaphoreType.DMA
        hbm, vmem = pl.BlockSpec(memory_space=pl.ANY), pl.BlockSpec(memory_space=pltpu.VMEM)
        return pl.pallas_call(
            _layer,
            out_shape=jax.ShapeDtypeStruct((rows, d), bf),
            in_specs=[hbm] + [vmem] * 5 + [hbm] * 4,
            out_specs=hbm,
            scratch_shapes=[
                pltpu.VMEM(wq.shape, bf),
                pltpu.VMEM((d, 2 * kv * HEAD), bf),
                pltpu.VMEM((wo.shape[0], half), bf),
                pltpu.VMEM((wo.shape[0], half), bf),
                pltpu.VMEM((2, ROWS, d), bf),
                pltpu.VMEM((2, ROWS, half), bf),
                pltpu.VMEM((ROWS, d), bf),
                pltpu.VMEM((kv, cols, HEAD), bf),
                pltpu.VMEM((kv, rows, HEAD), bf),
                pltpu.VMEM((kv, HEAD + 16, rows), bf),
                pltpu.VMEM((kv, cols), f32),
                pltpu.VMEM((kv, HEAD + 16, cols), f32),
                pltpu.VMEM((ROWS, heads * HEAD), bf),
                pltpu.VMEM((ROWS, half), f32),
                pltpu.VMEM((ROWS, half), bf),
                pltpu.VMEM((ROWS, half), bf),
                pltpu.VMEM((chunks, ROWS, half), bf),
                pltpu.VMEM((chunks, ROWS, half), bf),
                dma((n_weights,)),
                dma((2,)),
                dma((2,)),
                dma,
                dma,
                pltpu.SemaphoreType.REGULAR,
                dma((chunks,)),
                dma((chunks,)),
                dma((chunks,)),
                dma((chunks,)),
                dma((chunks,)),
            ],
            compiler_params=pltpu.CompilerParams(collective_id=0, has_side_effects=True, vmem_limit_bytes=VMEM),
        )(x, gain.reshape(1, d), *_tables(ROWS, chunks), wq, wk, wv, wo)

    tokens, columns = P("dp", None), P(None, "tp")
    return jax.shard_map(
        step,
        mesh=mesh,
        in_specs=(tokens, P(None), columns, columns, columns, P("tp", None)),
        out_specs=tokens,
        check_vma=False,
    )
```

```python
import jax
import jax.numpy as jnp
import numpy as np
from jax import lax
from jax.experimental import pallas as pl
from jax.experimental.pallas import tpu as pltpu
from jax.sharding import PartitionSpec as P

HEAD = 128
THETA = 10000
LOG2E = 1.4426950408889634
HIDDEN = -2e30
SMALL = 128
ROWS = 256
WIDE = 512
STRIP = 512
LAG = 2
MESH = pl.DeviceIdType.MESH
VMEM = 67_043_328


def _dot(a, b, ca, cb):
    return lax.dot_general(a, b, (((ca,), (cb,)), ((), ())), preferred_element_type=jnp.float32)


def _tables(rows):
    half = HEAD // 2
    rate = THETA ** (-np.arange(half, dtype=np.float64) / half)
    rate = np.concatenate([rate, rate])
    a = np.arange(ROWS)[:, None] * rate
    b = (np.arange(rows // SMALL) * SMALL)[:, None] * rate
    return [t.astype(np.float32) for t in (np.cos(a), np.sin(a), np.cos(b), np.sin(b))]


def _layer(x, gain, cos_a, sin_a, cos_b, sin_b, wq, wk, wv, wo, out,
           gain_s, cos_a_s, sin_a_s, cos_b_s, sin_b_s, wq_s, wkv_s, wo_far, wo_near, a_s, res_s, q_s, k_s, v_s, top_s, wide_s, seen_s,
           far_s, got_s, sum_s, peer_s,
           w_sem, in_sem, x_sem, res_sem, far_send, far_recv, free, sum_send, sum_recv, put_sem, give_send, give_recv):
    t = lax.axis_index("tp")
    core = lax.rem(t, 2)
    sibling = {"tp": t + 1 - 2 * core}
    partner = {"tp": lax.rem(t + 2, 4)}
    total_rows, d = x.shape
    last = (total_rows - 2 * SMALL) // ROWS + 1
    half = d // 2
    kv = k_s.shape[0]
    heads = wq.shape[1] // HEAD
    group = heads // kv
    near_cols = pl.ds(pl.multiple_of(core * half, half), half)
    nq, nk, no = wq.shape[1] // WIDE, wk.shape[1], half // WIDE
    e = HEAD**-0.5 * LOG2E

    def place(c):
        return SMALL + (c - 1) * ROWS

    def span(o, rows):
        return pl.ds(o if isinstance(o, int) else pl.multiple_of(o, SMALL), rows)

    def block_cols(side, n):
        return pl.ds(pl.multiple_of(side * half + n * WIDE, WIDE), WIDE)

    def static_cols(n):
        return pl.ds(n * WIDE, WIDE)

    weights = [(wk, wkv_s.at[:, pl.ds(0, nk)]), (wv, wkv_s.at[:, pl.ds(nk, nk)])]
    weights += [(wq.at[:, static_cols(n)], wq_s.at[:, static_cols(n)]) for n in range(nq)]
    weights += [(wo.at[:, block_cols(1 - core, n)], wo_far.at[:, static_cols(n)]) for n in range(no)]
    weights += [(wo.at[:, block_cols(core, n)], wo_near.at[:, static_cols(n)]) for n in range(no)]
    weights = [pltpu.make_async_copy(src, dst, w_sem.at[n]) for n, (src, dst) in enumerate(weights)]
    q_at, far_at, near_at = 2, 2 + nq, 2 + nq + no
    small = [(gain, gain_s), (cos_a, cos_a_s), (sin_a, sin_a_s), (cos_b, cos_b_s), (sin_b, sin_b_s)]
    small = [pltpu.make_async_copy(src, dst, in_sem.at[n]) for n, (src, dst) in enumerate(small)]

    def x_copy(o, rows):
        return pltpu.make_async_copy(x.at[span(o, rows), :], a_s.at[pl.ds(0, rows), :], x_sem)

    def res_copy(o, rows):
        return pltpu.make_async_copy(x.at[span(o, rows), near_cols], res_s.at[pl.ds(0, rows), :], res_sem)

    def far_copy(rows):
        at = pl.ds(0, rows)
        return pltpu.make_async_remote_copy(src_ref=far_s.at[at, :], dst_ref=got_s.at[at, :], send_sem=far_send, recv_sem=far_recv,
                                            device_id=sibling, device_id_type=MESH)

    def sum_copy(c, o, rows):
        return pltpu.make_async_remote_copy(src_ref=sum_s.at[span(o, rows), :], dst_ref=peer_s.at[span(o, rows), :], send_sem=sum_send.at[c],
                                            recv_sem=sum_recv.at[c], device_id=partner, device_id_type=MESH)

    def put_copy(c, o, rows):
        return pltpu.make_async_copy(sum_s.at[span(o, rows), :], out.at[span(o, rows), near_cols], put_sem.at[c])

    def give_copy(c, o, rows):
        return pltpu.make_async_remote_copy(src_ref=sum_s.at[span(o, rows), :], dst_ref=out.at[span(o, rows), near_cols], send_sem=give_send.at[c],
                                            recv_sem=give_recv.at[c], device_id=sibling, device_id_type=MESH)

    def by_rows(rows, unroll, body):
        @pl.loop(0, rows // 16, unroll=unroll)
        def _(r):
            body(pl.multiple_of(r * 16, 16))

    def finish(c, o, rows):
        with jax.named_scope("arrive"):
            res_copy(o, rows).wait()
            sum_copy(c, o, rows).wait()

        def add(r):
            here = pl.ds(pl.multiple_of(o + r, 16), 16)
            term = sum_s[here, :].astype(jnp.float32) + peer_s[here, :].astype(jnp.float32)
            sum_s[here, :] = (res_s[pl.ds(r, 16), :].astype(jnp.float32) + term).astype(jnp.bfloat16)

        by_rows(rows, 2, add)
        put_copy(c, o, rows).start()
        give_copy(c, o, rows).start()

    def attend(o, rows, first):
        cols = group * rows
        strip = max(n for n in range(rows, STRIP + 1, rows) if cols % n == 0)
        pieces = [(i, at) for i in range(kv) for at in range(0, cols, strip)]

        def block(at_key, keys, diagonal):
            here = span(at_key, keys)
            scores = [_dot(k_s[i, here, :], q_s[i, at : at + strip, :], 1, 1) for i, at in pieces]
            if diagonal:
                key = lax.broadcasted_iota(jnp.int32, (keys, strip), 0)
                query = lax.rem(lax.broadcasted_iota(jnp.int32, (keys, strip), 1), rows)
                ok = query >= key
            probs, keeps = [], []
            for (i, at), s in zip(pieces, scores):
                there = pl.ds(at, strip)
                if diagonal:
                    s = jnp.where(ok, s, HIDDEN)
                    top = s.max(axis=0, keepdims=True)
                else:
                    old = top_s[i : i + 1, there]
                    top = jnp.maximum(old, s.max(axis=0, keepdims=True))
                    keeps.append(jnp.exp2((old - top) * e))
                top_s[i : i + 1, there] = top
                probs.append(jnp.exp2((s - top) * e).astype(jnp.bfloat16))
            for n, ((i, at), p) in enumerate(zip(pieces, probs)):
                there = pl.ds(at, strip)
                new = _dot(v_s[i, :, here], p, 1, 0)
                deep = pl.ds(i * (HEAD + 16), HEAD + 16)
                wide_s[deep, there] = new if diagonal else wide_s[deep, there] * keeps[n] + new

        block(o, rows, True)
        if not first:
            block(0, SMALL, False)

            @pl.loop(0, lax.div(o - SMALL, ROWS))
            def _(j):
                block(SMALL + j * ROWS, ROWS, False)

        for i in range(kv):
            for n in range(group):
                there = pl.ds(n * rows, rows)
                h = i * group + n
                top = i * (HEAD + 16)
                done = wide_s[top : top + HEAD, there] * (1 / wide_s[top + HEAD : top + HEAD + 1, there])
                seen_s[pl.ds(0, rows), h * HEAD : (h + 1) * HEAD] = done.T.astype(jnp.bfloat16)

    def chunk(c, o, rows, first=False, after_q=None):
        at = pl.ds(0, rows)
        with jax.named_scope("x_wait"):
            x_copy(o, rows).wait()
            if first:
                for n in range(1, nq):
                    weights[q_at + n].start()
                for s in small:
                    s.wait()

        with jax.named_scope("norm"):
            def norm(r):
                wide = a_s[pl.ds(r, 16), :].astype(jnp.float32)
                scale = lax.rsqrt(jnp.mean(wide * wide, -1, keepdims=True) + 1e-6)
                a_s[pl.ds(r, 16), :] = (wide * scale * gain_s[...].astype(jnp.float32)).astype(jnp.bfloat16)

            by_rows(rows, 4, norm)
        if first:
            for n in range(no):
                weights[far_at + n].start()

        sign = jnp.where(lax.broadcasted_iota(jnp.int32, (rows, HEAD), 1) < HEAD // 2, -1.0, 1.0)
        ca, sa = cos_a_s[at, :], sin_a_s[at, :]
        cb, sb = (ref[pl.ds(0 if first else lax.div(o, SMALL), 1), :] for ref in (cos_b_s, sin_b_s))
        cos = ca * cb - sa * sb
        sin = (sa * cb + ca * sb) * sign

        def turned(u):
            u = u.astype(jnp.float32)
            return (u * cos + pltpu.roll(u, HEAD // 2, 1) * sin).astype(jnp.bfloat16)

        with jax.named_scope("kv"):
            if first:
                weights[0].wait()
                weights[1].wait()
            both = _dot(a_s[at, :], wkv_s[...], 1, 0).astype(jnp.bfloat16)
            for i in range(kv):
                k_s[i, span(o, rows), :] = turned(both[:, i * HEAD : (i + 1) * HEAD])
                v_s[i, :HEAD, span(o, rows)] = both[:, nk + i * HEAD : nk + (i + 1) * HEAD].T
        if first:
            for n in range(no):
                weights[near_at + n].start()
        with jax.named_scope("q"):
            for n in range(nq):
                if first:
                    weights[q_at + n].wait()
                part = _dot(a_s[at, :], wq_s[:, n * WIDE : (n + 1) * WIDE], 1, 0).astype(jnp.bfloat16)
                for m in range(WIDE // HEAD):
                    h = n * (WIDE // HEAD) + m
                    q_s[h // group, pl.ds((h % group) * rows, rows), :] = turned(part[:, m * HEAD : (m + 1) * HEAD])

        after_q()

        with jax.named_scope("attend"):
            attend(o, rows, first)

        if first:
            pl.semaphore_wait(pltpu.get_barrier_semaphore(), 2)
        else:
            pl.semaphore_wait(free, 1)
        with jax.named_scope("far"):
            for n in range(no):
                if first:
                    weights[far_at + n].wait()
                far_s[at, n * WIDE : (n + 1) * WIDE] = _dot(seen_s[at, :], wo_far[:, n * WIDE : (n + 1) * WIDE], 1, 0).astype(jnp.bfloat16)
            far_copy(rows).start()
        with jax.named_scope("near"):
            for n in range(no):
                if first:
                    weights[near_at + n].wait()
                wide_s[at, n * WIDE : (n + 1) * WIDE] = _dot(seen_s[at, :], wo_near[:, n * WIDE : (n + 1) * WIDE], 1, 0)
        with jax.named_scope("far_wait"):
            far_copy(rows).wait()

        with jax.named_scope("sum"):
            def add(r):
                near = wide_s[pl.ds(r, 16), :] + got_s[pl.ds(r, 16), :].astype(jnp.float32)
                sum_s[pl.ds(pl.multiple_of(o + r, 16), 16), :] = near.astype(jnp.bfloat16)

            by_rows(rows, 2, add)
        sum_copy(c, o, rows).start()

    x_copy(0, SMALL).start()
    for s in small:
        s.start()
    for w in weights[: q_at + 1]:
        w.start()
    barrier = pltpu.get_barrier_semaphore()
    for other in (sibling, partner):
        pl.semaphore_signal(barrier, inc=1, device_id=other, device_id_type=MESH)
    for i in range(kv):
        v_s[i, HEAD:, :] = jnp.ones((v_s.shape[1] - HEAD, v_s.shape[2]), v_s.dtype)

    def more():
        pl.semaphore_signal(free, inc=1, device_id=sibling, device_id_type=MESH)

    chunk(0, 0, SMALL, first=True, after_q=lambda: x_copy(SMALL, ROWS).start())
    more()

    @pl.loop(1, last)
    def _(c):
        o = place(c)

        @pl.when(c > LAG)
        def _():
            res_copy(place(c - LAG), ROWS).start()

        def after_q():
            @pl.when(c + 1 < last)
            def _():
                x_copy(o + ROWS, ROWS).start()

            @pl.when(c + 1 == last)
            def _():
                x_copy(o + ROWS, SMALL).start()

        chunk(c, o, ROWS, after_q=after_q)
        more()

        @pl.when(c > LAG)
        def _():
            finish(c - LAG, place(c - LAG), ROWS)

    end = total_rows - SMALL
    res_copy(0, SMALL).start()
    chunk(last, end, SMALL, after_q=lambda: None)
    finish(0, 0, SMALL)
    for f in range(last - LAG, last):
        res_copy(place(f), ROWS).start()
        finish(f, place(f), ROWS)
    res_copy(end, SMALL).start()
    finish(last, end, SMALL)

    for f in range(last + 1):
        o, rows = (place(f), ROWS) if 0 < f < last else (0 if f == 0 else end, SMALL)
        put_copy(f, o, rows).wait()
        give_copy(f, o, rows).wait()


def solution(mesh):
    def step(x, gain, wq, wk, wv, wo):
        rows, d = x.shape
        chunks = (rows - 2 * SMALL) // ROWS + 2
        kv = wk.shape[1] // HEAD
        heads = wq.shape[1] // HEAD
        cols = heads // kv * ROWS
        half = d // 2
        bf, f32 = jnp.bfloat16, jnp.float32
        tables = _tables(rows)
        n_weights = 2 + wq.shape[1] // WIDE + d // WIDE
        dma = pltpu.SemaphoreType.DMA
        hbm = pl.BlockSpec(memory_space=pl.ANY)
        return pl.pallas_call(
            _layer,
            out_shape=jax.ShapeDtypeStruct((rows, d), bf),
            in_specs=[hbm] * 10,
            out_specs=hbm,
            scratch_shapes=[
                pltpu.VMEM(gain.shape, bf),
                *[pltpu.VMEM(t.shape, f32) for t in tables],
                pltpu.VMEM(wq.shape, bf),
                pltpu.VMEM((d, 2 * kv * HEAD), bf),
                pltpu.VMEM((wo.shape[0], half), bf),
                pltpu.VMEM((wo.shape[0], half), bf),
                pltpu.VMEM((ROWS, d), bf),
                pltpu.VMEM((ROWS, half), bf),
                pltpu.VMEM((kv, cols, HEAD), bf),
                pltpu.VMEM((kv, rows, HEAD), bf),
                pltpu.VMEM((kv, HEAD + 16, rows), bf),
                pltpu.VMEM((kv, cols), f32),
                pltpu.VMEM((max(kv * (HEAD + 16), ROWS), max(cols, half)), f32),
                pltpu.VMEM((ROWS, heads * HEAD), bf),
                pltpu.VMEM((ROWS, half), bf),
                pltpu.VMEM((ROWS, half), bf),
                pltpu.VMEM((rows, half), bf),
                pltpu.VMEM((rows, half), bf),
                dma((n_weights,)),
                dma((5,)),
                dma,
                dma,
                dma,
                dma,
                pltpu.SemaphoreType.REGULAR,
                dma((chunks,)),
                dma((chunks,)),
                dma((chunks,)),
                dma((chunks,)),
                dma((chunks,)),
            ],
            compiler_params=pltpu.CompilerParams(collective_id=0, has_side_effects=True, vmem_limit_bytes=VMEM),
        )(x, gain, *tables, wq, wk, wv, wo)

    tokens, columns = P("dp", None), P(None, "tp")
    return jax.shard_map(
        step,
        mesh=mesh,
        in_specs=(tokens, P(None), columns, columns, columns, P("tp", None)),
        out_specs=tokens,
        check_vma=False,
    )
```

```python
import jax
import jax.numpy as jnp
import numpy as np
from jax import lax
from jax.experimental import pallas as pl
from jax.experimental.pallas import tpu as pltpu
from jax.sharding import PartitionSpec as P


HEAD = 128
THETA = 10000
LOG2E = 1.4426950408889634
HIDDEN = -2e30
SMALL = 128
ROWS = 256
WIDE = 512
STRIP = 512
LAG = 2
CLOSE = 64
LATE = 2
MESH = pl.DeviceIdType.MESH
VMEM = 67_043_328


def _dot(a, b, ca, cb):
    return lax.dot_general(a, b, (((ca,), (cb,)), ((), ())), preferred_element_type=jnp.float32)


def _tables(rows):
    half = HEAD // 2
    rate = THETA ** (-np.arange(half, dtype=np.float64) / half)
    rate = np.concatenate([rate, rate])
    a = np.arange(ROWS)[:, None] * rate
    b = (np.arange(rows // SMALL) * SMALL)[:, None] * rate
    return [t.astype(np.float32) for t in (np.cos(a), np.sin(a), np.cos(b), np.sin(b))]


def _layer(x, gain, cos_a, sin_a, cos_b, sin_b, wq, wk, wv, wo, out, crossed, *rest):
    sums, late, rest = rest[: LATE + 1], rest[LATE + 1 : 2 * LATE + 1], rest[2 * LATE + 1 :]
    _run(x, gain, cos_a, sin_a, cos_b, sin_b, wq, wk, wv, wo, out, sums, crossed, late, *rest)


def _run(x, gain, cos_a, sin_a, cos_b, sin_b, wq, wk, wv, wo, out, sums, crossed, late,
           gain_s, cos_a_s, sin_a_s, cos_b_s, sin_b_s, wq_s, wkv_s, wo_far, wo_near, a_s, res_s, q_s, k_s, v_s, top_s, wide_s, seen_s,
           far_s, got_s, sum_s, peer_s,
           w_sem, in_sem, x_sem, res_sem, far_send, far_recv, free, sum_send, sum_recv, put_sem, give_send, give_recv, late_sem):
    t = lax.axis_index("tp")
    core = lax.rem(t, 2)
    sibling = {"tp": t + 1 - 2 * core}
    partner = {"tp": lax.rem(t + 2, 4)}
    total_rows, d = x.shape
    last = (total_rows - 2 * SMALL) // ROWS + 1
    edge = last - LATE
    half = d // 2
    kv = k_s.shape[0]
    heads = wq.shape[1] // HEAD
    group = heads // kv
    near_cols = pl.ds(pl.multiple_of(core * half, half), half)
    nq, nk, no = wq.shape[1] // WIDE, wk.shape[1], half // WIDE
    e = HEAD**-0.5 * LOG2E

    def place(c):
        return SMALL + (c - 1) * ROWS

    def span(o, rows):
        return pl.ds(o if isinstance(o, int) else pl.multiple_of(o, SMALL), rows)

    def block_cols(side, n):
        return pl.ds(pl.multiple_of(side * half + n * WIDE, WIDE), WIDE)

    def static_cols(n):
        return pl.ds(n * WIDE, WIDE)

    weights = [(wk, wkv_s.at[:, pl.ds(0, nk)]), (wv, wkv_s.at[:, pl.ds(nk, nk)])]
    weights += [(wq.at[:, static_cols(n)], wq_s.at[:, static_cols(n)]) for n in range(nq)]
    weights += [(wo.at[:, block_cols(1 - core, n)], wo_far.at[:, static_cols(n)]) for n in range(no)]
    weights += [(wo.at[:, block_cols(core, n)], wo_near.at[:, static_cols(n)]) for n in range(no)]
    weights = [pltpu.make_async_copy(src, dst, w_sem.at[n]) for n, (src, dst) in enumerate(weights)]
    q_at, far_at, near_at = 2, 2 + nq, 2 + nq + no
    small = [(gain, gain_s), (cos_a, cos_a_s), (sin_a, sin_a_s), (cos_b, cos_b_s), (sin_b, sin_b_s)]
    small = [pltpu.make_async_copy(src, dst, in_sem.at[n]) for n, (src, dst) in enumerate(small)]

    def x_copy(o, rows):
        return pltpu.make_async_copy(x.at[span(o, rows), :], a_s.at[pl.ds(0, rows), :], x_sem)

    def res_copy(o, rows):
        return pltpu.make_async_copy(x.at[span(o, rows), near_cols], res_s.at[pl.ds(0, rows), :], res_sem)

    def far_copy(rows):
        at = pl.ds(0, rows)
        return pltpu.make_async_remote_copy(src_ref=far_s.at[at, :], dst_ref=got_s.at[at, :], send_sem=far_send, recv_sem=far_recv,
                                            device_id=sibling, device_id_type=MESH)

    def sum_copy(c, o, rows, target):
        return pltpu.make_async_remote_copy(src_ref=sum_s.at[span(o, rows), :], dst_ref=target, send_sem=sum_send.at[c],
                                            recv_sem=sum_recv.at[c], device_id=partner, device_id_type=MESH)

    def peer_copy(c, o, rows):
        return sum_copy(c, o, rows, peer_s.at[span(o, rows), :])

    def edge_copy():
        return sum_copy(edge, place(edge), ROWS, crossed)

    def put_copy(c, o, rows, target):
        return pltpu.make_async_copy(sum_s.at[span(o, rows), :], target, put_sem.at[c])

    def give_copy(c, o, rows, target):
        return pltpu.make_async_remote_copy(src_ref=sum_s.at[span(o, rows), :], dst_ref=target, send_sem=give_send.at[c],
                                            recv_sem=give_recv.at[c], device_id=sibling, device_id_type=MESH)

    def spread(c, o, rows):
        done = isinstance(c, jax.Array) or c < edge
        target = out.at[span(o, rows), near_cols] if done else sums[c - edge].at[:, near_cols]
        return put_copy(c, o, rows, target), give_copy(c, o, rows, target)

    def late_copy(n, o, rows):
        return pltpu.make_async_copy(sum_s.at[span(o, rows), :], late[n], late_sem.at[n])

    def by_rows(rows, unroll, body):
        @pl.loop(0, rows // 16, unroll=unroll)
        def _(r):
            body(pl.multiple_of(r * 16, 16))

    def finish(c, o, rows):
        res_copy(o, rows).wait()
        peer_copy(c, o, rows).wait()

        def add(r):
            here = pl.ds(pl.multiple_of(o + r, 16), 16)
            term = sum_s[here, :].astype(jnp.float32) + peer_s[here, :].astype(jnp.float32)
            sum_s[here, :] = (res_s[pl.ds(r, 16), :].astype(jnp.float32) + term).astype(jnp.bfloat16)

        by_rows(rows, 2, add)
        for copy in spread(c, o, rows):
            copy.start()

    def attend(o, rows, first):
        cols = group * rows
        strip = max(n for n in range(rows, STRIP + 1, rows) if cols % n == 0)
        pieces = [(i, at) for i in range(kv) for at in range(0, cols, strip)]

        def block(at_key, keys, diagonal):
            here = span(at_key, keys)
            scores = [_dot(k_s[i, here, :], q_s[i, at : at + strip, :], 1, 1) for i, at in pieces]
            if diagonal:
                key = lax.broadcasted_iota(jnp.int32, (keys, strip), 0)
                query = lax.rem(lax.broadcasted_iota(jnp.int32, (keys, strip), 1), rows)
                ok = query >= key
            probs, keeps = [], []
            for (i, at), s in zip(pieces, scores):
                there = pl.ds(at, strip)
                if diagonal:
                    s = jnp.where(ok, s, HIDDEN)
                    top = s.max(axis=0, keepdims=True)
                else:
                    old = top_s[i : i + 1, there]
                    top = jnp.maximum(old, s.max(axis=0, keepdims=True))
                    keeps.append(jnp.exp2((old - top) * e))
                top_s[i : i + 1, there] = top
                probs.append(jnp.exp2((s - top) * e).astype(jnp.bfloat16))
            for n, ((i, at), p) in enumerate(zip(pieces, probs)):
                there = pl.ds(at, strip)
                new = _dot(v_s[i, :, here], p, 1, 0)
                deep = pl.ds(i * (HEAD + 16), HEAD + 16)
                wide_s[deep, there] = new if diagonal else wide_s[deep, there] * keeps[n] + new

        block(o, rows, True)
        if not first:
            block(0, SMALL, False)

            @pl.loop(0, lax.div(o - SMALL, ROWS))
            def _(j):
                block(SMALL + j * ROWS, ROWS, False)

        for i in range(kv):
            for n in range(group):
                there = pl.ds(n * rows, rows)
                h = i * group + n
                top = i * (HEAD + 16)
                done = wide_s[top : top + HEAD, there] * (1 / wide_s[top + HEAD : top + HEAD + 1, there])
                seen_s[pl.ds(0, rows), h * HEAD : (h + 1) * HEAD] = done.T.astype(jnp.bfloat16)

    def chunk(o, rows, first=False, after_q=None):
        at = pl.ds(0, rows)
        x_copy(o, rows).wait()
        if first:
            for n in range(1, nq):
                weights[q_at + n].start()
            for s in small:
                s.wait()

        def norm(r):
            wide = a_s[pl.ds(r, 16), :].astype(jnp.float32)
            scale = lax.rsqrt(jnp.mean(wide * wide, -1, keepdims=True) + 1e-6)
            a_s[pl.ds(r, 16), :] = (wide * scale * gain_s[...].astype(jnp.float32)).astype(jnp.bfloat16)

        by_rows(rows, 4, norm)
        if first:
            for n in range(no):
                weights[far_at + n].start()

        sign = jnp.where(lax.broadcasted_iota(jnp.int32, (rows, HEAD), 1) < HEAD // 2, -1.0, 1.0)
        ca, sa = cos_a_s[at, :], sin_a_s[at, :]
        cb, sb = (ref[pl.ds(0 if first else lax.div(o, SMALL), 1), :] for ref in (cos_b_s, sin_b_s))
        cos = ca * cb - sa * sb
        sin = (sa * cb + ca * sb) * sign

        def turned(u):
            u = u.astype(jnp.float32)
            return (u * cos + pltpu.roll(u, HEAD // 2, 1) * sin).astype(jnp.bfloat16)

        if first:
            weights[0].wait()
            weights[1].wait()
        both = _dot(a_s[at, :], wkv_s[...], 1, 0).astype(jnp.bfloat16)
        for i in range(kv):
            k_s[i, span(o, rows), :] = turned(both[:, i * HEAD : (i + 1) * HEAD])
            v_s[i, :HEAD, span(o, rows)] = both[:, nk + i * HEAD : nk + (i + 1) * HEAD].T
        if first:
            for n in range(no):
                weights[near_at + n].start()
        for n in range(nq):
            if first:
                weights[q_at + n].wait()
            part = _dot(a_s[at, :], wq_s[:, n * WIDE : (n + 1) * WIDE], 1, 0).astype(jnp.bfloat16)
            for m in range(WIDE // HEAD):
                h = n * (WIDE // HEAD) + m
                q_s[h // group, pl.ds((h % group) * rows, rows), :] = turned(part[:, m * HEAD : (m + 1) * HEAD])

        after_q()

        attend(o, rows, first)

        if first:
            pl.semaphore_wait(pltpu.get_barrier_semaphore(), 2)
        else:
            pl.semaphore_wait(free, 1)
        for n in range(no):
            if first:
                weights[far_at + n].wait()
            far_s[at, n * WIDE : (n + 1) * WIDE] = _dot(seen_s[at, :], wo_far[:, n * WIDE : (n + 1) * WIDE], 1, 0).astype(jnp.bfloat16)
        far_copy(rows).start()
        for n in range(no):
            if first:
                weights[near_at + n].wait()
            wide_s[at, n * WIDE : (n + 1) * WIDE] = _dot(seen_s[at, :], wo_near[:, n * WIDE : (n + 1) * WIDE], 1, 0)
        far_copy(rows).wait()

        def add(r):
            near = wide_s[pl.ds(r, 16), :] + got_s[pl.ds(r, 16), :].astype(jnp.float32)
            sum_s[pl.ds(pl.multiple_of(o + r, 16), 16), :] = near.astype(jnp.bfloat16)

        by_rows(rows, 2, add)

    x_copy(0, SMALL).start()
    for s in small:
        s.start()
    for w in weights[: q_at + 1]:
        w.start()
    barrier = pltpu.get_barrier_semaphore()
    for other in (sibling, partner):
        pl.semaphore_signal(barrier, inc=1, device_id=other, device_id_type=MESH)
    for i in range(kv):
        v_s[i, HEAD:, :] = jnp.ones((v_s.shape[1] - HEAD, v_s.shape[2]), v_s.dtype)

    def more():
        pl.semaphore_signal(free, inc=1, device_id=sibling, device_id_type=MESH)

    chunk(0, SMALL, first=True, after_q=lambda: x_copy(SMALL, ROWS).start())
    peer_copy(0, 0, SMALL).start()
    more()

    @pl.loop(1, last)
    def _(c):
        o = place(c)

        @pl.when(c > LAG)
        def _():
            res_copy(place(c - LAG), ROWS).start()

        def after_q():
            @pl.when(c + 1 < last)
            def _():
                x_copy(o + ROWS, ROWS).start()

            @pl.when(c + 1 == last)
            def _():
                x_copy(o + ROWS, SMALL).start()

        chunk(o, ROWS, after_q=after_q)
        more()

        @pl.when(c < edge)
        def _():
            peer_copy(c, o, ROWS).start()

        @pl.when(c == edge)
        def _():
            edge_copy().start()

        for f in range(edge, last):

            @pl.when(c == f)
            def _():
                for copy in spread(f, place(f), ROWS):
                    copy.start()
                if f > edge:
                    late_copy(f - edge - 1, place(f), ROWS).start()

        @pl.when(c > LAG)
        def _():
            finish(c - LAG, place(c - LAG), ROWS)

    end = total_rows - SMALL
    res_copy(0, SMALL).start()
    chunk(end, SMALL, after_q=lambda: None)
    for copy in spread(last, end, SMALL):
        copy.start()
    late_copy(LATE - 1, end, SMALL).start()
    finish(0, 0, SMALL)

    for f in range(last + 1):
        o, rows = (place(f), ROWS) if 0 < f < last else (0 if f == 0 else end, SMALL)
        for copy in spread(f, o, rows):
            copy.wait()
        if f > edge:
            late_copy(f - edge - 1, o, rows).wait()
    edge_copy().wait()


def _copied(done, y, buf, in_sem, out_sem):
    steps, rows = buf.shape[:2]
    here = lambda n: pl.ds(n * rows, rows)
    reads = [pltpu.make_async_copy(done.at[here(n), :], buf.at[n], in_sem.at[n]) for n in range(steps)]
    writes = [pltpu.make_async_copy(buf.at[n], y.at[here(n), :], out_sem.at[n]) for n in range(steps)]
    for copy in reads:
        copy.start()
    for read, write in zip(reads, writes):
        read.wait()
        write.start()
    for copy in writes:
        copy.wait()


def _closed(x, sums, own, other, old, y):
    first = lax.rem(lax.axis_index("tp"), 2) == 0
    half = own.shape[1]
    here = pl.ds(pl.multiple_of(pl.program_id(0) * y.shape[0], y.shape[0]), y.shape[0])
    for n in range(2):
        cols = slice(n * half, (n + 1) * half)
        mine = first if n == 0 else jnp.logical_not(first)

        def add(ref):
            term = sums[here, cols].astype(jnp.float32) + ref[here, :].astype(jnp.float32)
            y[:, cols] = (x[here, cols].astype(jnp.float32) + term).astype(y.dtype)

        pl.when(mine)(lambda: add(own))
        pl.when(jnp.logical_not(mine))(lambda: add(other))


def solution(mesh):
    def layer(x, gain, wq, wk, wv, wo):
        rows, d = x.shape
        chunks = (rows - 2 * SMALL) // ROWS + 2
        kv = wk.shape[1] // HEAD
        heads = wq.shape[1] // HEAD
        cols = heads // kv * ROWS
        half = d // 2
        bf, f32 = jnp.bfloat16, jnp.float32
        tables = _tables(rows)
        n_weights = 2 + wq.shape[1] // WIDE + d // WIDE
        dma = pltpu.SemaphoreType.DMA
        hbm = pl.BlockSpec(memory_space=pl.ANY)
        done = rows - SMALL - (LATE - 1) * ROWS - ROWS
        sizes = [ROWS] * LATE + [SMALL]
        out, crossed, *more = pl.pallas_call(
            _layer,
            out_shape=[
                jax.ShapeDtypeStruct((done, d), bf),
                jax.ShapeDtypeStruct((ROWS, half), bf),
                *[jax.ShapeDtypeStruct((n, d), bf) for n in sizes],
                *[jax.ShapeDtypeStruct((n, half), bf) for n in sizes[1:]],
            ],
            in_specs=[hbm] * 10,
            out_specs=[hbm] * (3 + 2 * LATE),
            scratch_shapes=[
                pltpu.VMEM(gain.shape, bf),
                *[pltpu.VMEM(t.shape, f32) for t in tables],
                pltpu.VMEM(wq.shape, bf),
                pltpu.VMEM((d, 2 * kv * HEAD), bf),
                pltpu.VMEM((wo.shape[0], half), bf),
                pltpu.VMEM((wo.shape[0], half), bf),
                pltpu.VMEM((ROWS, d), bf),
                pltpu.VMEM((ROWS, half), bf),
                pltpu.VMEM((kv, cols, HEAD), bf),
                pltpu.VMEM((kv, rows, HEAD), bf),
                pltpu.VMEM((kv, HEAD + 16, rows), bf),
                pltpu.VMEM((kv, cols), f32),
                pltpu.VMEM((max(kv * (HEAD + 16), ROWS), max(cols, half)), f32),
                pltpu.VMEM((ROWS, heads * HEAD), bf),
                pltpu.VMEM((ROWS, half), bf),
                pltpu.VMEM((ROWS, half), bf),
                pltpu.VMEM((rows, half), bf),
                pltpu.VMEM((done, half), bf),
                dma((n_weights,)),
                dma((5,)),
                dma,
                dma,
                dma,
                dma,
                pltpu.SemaphoreType.REGULAR,
                dma((chunks,)),
                dma((chunks,)),
                dma((chunks,)),
                dma((chunks,)),
                dma((chunks,)),
                dma((LATE,)),
            ],
            compiler_params=pltpu.CompilerParams(collective_id=0, has_side_effects=True, vmem_limit_bytes=VMEM),
        )(x, gain, *tables, wq, wk, wv, wo)

        def across(a):
            return lax.ppermute(a, "tp", [(i, (i + 2) % 4) for i in range(4)])

        def beside(a):
            return lax.ppermute(a, "tp", [(i, i ^ 1) for i in range(4)])

        sums, late = more[: LATE + 1], more[LATE + 1 :]
        arrived = [crossed]
        for n, a in enumerate(late):
            arrived.append(across(a))

        y = pl.pallas_call(
            _copied,
            out_shape=jax.ShapeDtypeStruct((rows, d), bf),
            in_specs=[hbm],
            out_specs=hbm,
            scratch_shapes=[pltpu.VMEM((done // SMALL, SMALL, d), bf), dma((done // SMALL,)), dma((done // SMALL,))],
            cost_estimate=pl.CostEstimate(flops=10**10, bytes_accessed=4 * done * d, transcendentals=0),
            compiler_params=pltpu.CompilerParams(vmem_limit_bytes=24 * 2**20),
        )(out)
        start = done
        vmem = pl.BlockSpec(memory_space=pltpu.VMEM)
        for own, term in zip(arrived, sums):
            n = own.shape[0]
            if start > done:
                own, y = lax.optimization_barrier((own, y))
            rows_x = lax.slice_in_dim(x, start, start + n)
            y = pl.pallas_call(
                _closed,
                out_shape=jax.ShapeDtypeStruct((rows, d), bf),
                grid=(n // CLOSE,),
                in_specs=[vmem] * 4 + [hbm],
                out_specs=pl.BlockSpec((CLOSE, d), lambda i, at=start // CLOSE: (at + i, 0)),
                input_output_aliases={4: 0},
                cost_estimate=pl.CostEstimate(flops=10**9, bytes_accessed=8 * n * d, transcendentals=0),
                compiler_params=pltpu.CompilerParams(vmem_limit_bytes=24 * 2**20),
            )(rows_x, term, own, beside(own), y)
            start += n
        return y

    tokens, columns = P("dp", None), P(None, "tp")
    return jax.shard_map(
        layer,
        mesh=mesh,
        in_specs=(tokens, P(None), columns, columns, columns, P("tp", None)),
        out_specs=tokens,
        check_vma=False,
    )
```

```python
import jax
import jax.numpy as jnp
import numpy as np
from jax import lax
from jax.experimental import pallas as pl
from jax.experimental.pallas import tpu as pltpu
from jax.sharding import PartitionSpec as P


HEAD = 128
THETA = 10000
LOG2E = 1.4426950408889634
HIDDEN = -2e30
SMALL = 128
FRONT = 4
ROWS = 256
WIDE = 512
STRIP = 512
LAG = 2
CLOSE = 64
LATE = 2
MESH = pl.DeviceIdType.MESH
VMEM = 67_043_328


def _dot(a, b, ca, cb):
    return lax.dot_general(a, b, (((ca,), (cb,)), ((), ())), preferred_element_type=jnp.float32)


def _tables(rows):
    half = HEAD // 2
    rate = THETA ** (-np.arange(half, dtype=np.float64) / half)
    rate = np.concatenate([rate, rate])
    a = np.arange(ROWS)[:, None] * rate
    b = (np.arange(rows // SMALL) * SMALL)[:, None] * rate
    return [t.astype(np.float32) for t in (np.cos(a), np.sin(a), np.cos(b), np.sin(b))]


def _layer(x, gain, cos_a, sin_a, cos_b, sin_b, wq, wk, wv, wo, out, crossed, *rest):
    sums, late, rest = rest[: LATE + 1], rest[LATE + 1 : 2 * LATE + 1], rest[2 * LATE + 1 :]
    _run(x, gain, cos_a, sin_a, cos_b, sin_b, wq, wk, wv, wo, out, sums, crossed, late, *rest)


def _run(x, gain, cos_a, sin_a, cos_b, sin_b, wq, wk, wv, wo, out, sums, crossed, late,
         gain_s, cos_a_s, sin_a_s, cos_b_s, sin_b_s, wq_s, wkv_s, wo_far, wo_near, x_s, a_s, res_s, q_s, k_s, v_s, top_s, wide_s, seen_s,
         far_s, got_s, sum_s, peer_s,
         w_sem, in_sem, x_sem, res_sem, far_send, far_recv, free, sum_send, sum_recv, put_sem, give_send, give_recv, late_sem, first_send, first_recv):
    t = lax.axis_index("tp")
    core = lax.rem(t, 2)
    sibling = {"tp": t + 1 - 2 * core}
    partner = {"tp": lax.rem(t + 2, 4)}
    total_rows, d = x.shape
    edge = (total_rows - (FRONT + LATE) * SMALL) // ROWS + FRONT - 1
    last = edge + LATE
    half = d // 2
    kv = k_s.shape[0]
    heads = wq.shape[1] // HEAD
    group = heads // kv
    near_cols = pl.ds(pl.multiple_of(core * half, half), half)
    nq, nk, no = wq.shape[1] // WIDE, wk.shape[1], half // WIDE
    e = HEAD**-0.5 * LOG2E

    def place(c):
        return FRONT * SMALL + (c - FRONT) * ROWS

    def shape(c):
        if FRONT <= c <= edge:
            return place(c), ROWS
        return (c * SMALL if c < FRONT else place(edge + 1) + (c - edge - 1) * SMALL), SMALL

    def span(o, rows):
        return pl.ds(o if isinstance(o, int) else pl.multiple_of(o, SMALL), rows)

    def block_cols(side, n):
        return pl.ds(pl.multiple_of(side * half + n * WIDE, WIDE), WIDE)

    def static_cols(n):
        return pl.ds(n * WIDE, WIDE)

    weights = [(wk, wkv_s.at[:, pl.ds(0, nk)]), (wv, wkv_s.at[:, pl.ds(nk, nk)])]
    weights += [(wq.at[:, static_cols(n)], wq_s.at[:, static_cols(n)]) for n in range(nq)]
    for n in range(no):
        weights += [(wo.at[:, block_cols(1 - core, n)], wo_far.at[:, static_cols(n)])]
        weights += [(wo.at[:, block_cols(core, n)], wo_near.at[:, static_cols(n)])]
    weights = [pltpu.make_async_copy(src, dst, w_sem.at[n]) for n, (src, dst) in enumerate(weights)]
    q_at, wo_at = 2, 2 + nq
    small = [(gain, gain_s), (cos_a, cos_a_s), (sin_a, sin_a_s), (cos_b, cos_b_s), (sin_b, sin_b_s)]
    small = [pltpu.make_async_copy(src, dst, in_sem.at[n]) for n, (src, dst) in enumerate(small)]

    def x_copy(o, rows):
        return pltpu.make_async_copy(x.at[span(o, rows), :], x_s.at[pl.ds(0, rows), :], x_sem)

    def res_copy(o, rows):
        return pltpu.make_async_copy(x.at[span(o, rows), near_cols], res_s.at[pl.ds(0, rows), :], res_sem)

    def far_copy(rows):
        at = pl.ds(0, rows)
        return pltpu.make_async_remote_copy(src_ref=far_s.at[at, :], dst_ref=got_s.at[at, :], send_sem=far_send, recv_sem=far_recv,
                                            device_id=sibling, device_id_type=MESH)

    def first_far(n):
        there = (pl.ds(0, SMALL), static_cols(n))
        return pltpu.make_async_remote_copy(src_ref=far_s.at[there], dst_ref=got_s.at[there], send_sem=first_send.at[0, n],
                                            recv_sem=first_recv.at[0, n], device_id=sibling, device_id_type=MESH)

    def first_sum(n):
        there = (pl.ds(0, SMALL), static_cols(n))
        return pltpu.make_async_remote_copy(src_ref=sum_s.at[there], dst_ref=peer_s.at[there], send_sem=first_send.at[1, n],
                                            recv_sem=first_recv.at[1, n], device_id=partner, device_id_type=MESH)

    def sum_copy(c, o, rows, target):
        return pltpu.make_async_remote_copy(src_ref=sum_s.at[span(o, rows), :], dst_ref=target, send_sem=sum_send.at[c],
                                            recv_sem=sum_recv.at[c], device_id=partner, device_id_type=MESH)

    def peer_copy(c, o, rows):
        return sum_copy(c, o, rows, peer_s.at[span(o, rows), :])

    def edge_copy():
        return sum_copy(edge, place(edge), ROWS, crossed)

    def put_copy(c, o, rows, target):
        return pltpu.make_async_copy(sum_s.at[span(o, rows), :], target, put_sem.at[c])

    def give_copy(c, o, rows, target):
        return pltpu.make_async_remote_copy(src_ref=sum_s.at[span(o, rows), :], dst_ref=target, send_sem=give_send.at[c],
                                            recv_sem=give_recv.at[c], device_id=sibling, device_id_type=MESH)

    def spread(c, o, rows):
        done = not isinstance(c, int) or c < edge
        target = out.at[span(o, rows), near_cols] if done else sums[c - edge].at[:, near_cols]
        return put_copy(c, o, rows, target), give_copy(c, o, rows, target)

    def late_copy(n, o, rows):
        return pltpu.make_async_copy(sum_s.at[span(o, rows), :], late[n], late_sem.at[n])

    def by_rows(rows, unroll, body):
        @pl.loop(0, rows // 16, unroll=unroll)
        def _(r):
            body(pl.multiple_of(r * 16, 16))

    def finish(c, o, rows):
        res_copy(o, rows).wait()
        if isinstance(c, int) and c == 0:
            for n in range(no):
                first_sum(n).wait()
        else:
            peer_copy(c, o, rows).wait()

        def add(r):
            here = pl.ds(pl.multiple_of(o + r, 16), 16)
            term = sum_s[here, :].astype(jnp.float32) + peer_s[here, :].astype(jnp.float32)
            sum_s[here, :] = (res_s[pl.ds(r, 16), :].astype(jnp.float32) + term).astype(jnp.bfloat16)

        by_rows(rows, 2, add)
        for copy in spread(c, o, rows):
            copy.start()

    def attend(o, rows):
        cols = group * rows
        strip = max(n for n in range(rows, STRIP + 1, rows) if cols % n == 0)
        pieces = [(i, at) for i in range(kv) for at in range(0, cols, strip)]

        def block(at_key, keys, diagonal):
            here = span(at_key, keys)
            scores = [_dot(k_s[i, here, :], q_s[i, at : at + strip, :], 1, 1) for i, at in pieces]
            if diagonal:
                key = lax.broadcasted_iota(jnp.int32, (keys, strip), 0)
                query = lax.rem(lax.broadcasted_iota(jnp.int32, (keys, strip), 1), rows)
                ok = query >= key
            probs, keeps = [], []
            for (i, at), s in zip(pieces, scores):
                there = pl.ds(at, strip)
                if diagonal:
                    s = jnp.where(ok, s, HIDDEN)
                    top = s.max(axis=0, keepdims=True)
                else:
                    old = top_s[i : i + 1, there]
                    top = jnp.maximum(old, s.max(axis=0, keepdims=True))
                    keeps.append(jnp.exp2((old - top) * e))
                top_s[i : i + 1, there] = top
                probs.append(jnp.exp2((s - top) * e).astype(jnp.bfloat16))
            for n, ((i, at), p) in enumerate(zip(pieces, probs)):
                there = pl.ds(at, strip)
                new = _dot(v_s[i, :, here], p, 1, 0)
                deep = pl.ds(i * (HEAD + 16), HEAD + 16)
                wide_s[deep, there] = new if diagonal else wide_s[deep, there] * keeps[n] + new

        block(o, rows, True)
        if isinstance(o, int):
            for k in range(0, o, SMALL):
                block(k, SMALL, False)
        else:

            @pl.loop(0, lax.div(o, ROWS))
            def _(j):
                block(j * ROWS, ROWS, False)

            if rows < ROWS:

                @pl.when(lax.rem(o, ROWS) > 0)
                def _():
                    block(o - SMALL, SMALL, False)

        for i in range(kv):
            for n in range(group):
                there = pl.ds(n * rows, rows)
                h = i * group + n
                top = i * (HEAD + 16)
                done = wide_s[top : top + HEAD, there] * (1 / wide_s[top + HEAD : top + HEAD + 1, there])
                seen_s[pl.ds(0, rows), h * HEAD : (h + 1) * HEAD] = done.T.astype(jnp.bfloat16)

    def chunk(o, rows, first=False, after_norm=None):
        at = pl.ds(0, rows)
        x_copy(o, rows).wait()
        if first:
            for n in range(1, nq):
                weights[q_at + n].start()
            for s in small:
                s.wait()

        def norm(r):
            wide = x_s[pl.ds(r, 16), :].astype(jnp.float32)
            scale = lax.rsqrt(jnp.mean(wide * wide, -1, keepdims=True) + 1e-6)
            a_s[pl.ds(r, 16), :] = (wide * scale * gain_s[...].astype(jnp.float32)).astype(jnp.bfloat16)

        by_rows(rows, 4, norm)
        after_norm()

        sign = jnp.where(lax.broadcasted_iota(jnp.int32, (rows, HEAD), 1) < HEAD // 2, -1.0, 1.0)
        ca, sa = cos_a_s[at, :], sin_a_s[at, :]
        cb, sb = (ref[pl.ds(o // SMALL if isinstance(o, int) else lax.div(o, SMALL), 1), :] for ref in (cos_b_s, sin_b_s))
        cos = ca * cb - sa * sb
        sin = (sa * cb + ca * sb) * sign

        def turned(u):
            u = u.astype(jnp.float32)
            return (u * cos + pltpu.roll(u, HEAD // 2, 1) * sin).astype(jnp.bfloat16)

        if first:
            weights[0].wait()
            weights[1].wait()
        both = _dot(a_s[at, :], wkv_s[...], 1, 0).astype(jnp.bfloat16)
        for i in range(kv):
            k_s[i, span(o, rows), :] = turned(both[:, i * HEAD : (i + 1) * HEAD])
            v_s[i, :HEAD, span(o, rows)] = both[:, nk + i * HEAD : nk + (i + 1) * HEAD].T
        for n in range(nq):
            if first:
                weights[q_at + n].wait()
                for w in weights[wo_at + 2 * n : wo_at + 2 * n + 2]:
                    w.start()
            part = _dot(a_s[at, :], wq_s[:, n * WIDE : (n + 1) * WIDE], 1, 0).astype(jnp.bfloat16)
            for m in range(WIDE // HEAD):
                h = n * (WIDE // HEAD) + m
                q_s[h // group, pl.ds((h % group) * rows, rows), :] = turned(part[:, m * HEAD : (m + 1) * HEAD])

        if first:
            for w in weights[wo_at + 2 * nq :]:
                w.start()
            x_copy(SMALL, SMALL).start()
        attend(o, rows)

        def far_block(n):
            cols = slice(n * WIDE, (n + 1) * WIDE)
            far_s[at, cols] = _dot(seen_s[at, :], wo_far[:, cols], 1, 0).astype(jnp.bfloat16)

        def near_block(n):
            cols = slice(n * WIDE, (n + 1) * WIDE)
            wide_s[at, cols] = _dot(seen_s[at, :], wo_near[:, cols], 1, 0)

        def add_up(cols):
            def add(r):
                near = wide_s[pl.ds(r, 16), cols] + got_s[pl.ds(r, 16), cols].astype(jnp.float32)
                sum_s[pl.ds(pl.multiple_of(o + r, 16), 16), cols] = near.astype(jnp.bfloat16)

            by_rows(rows, 2, add)

        if first:
            pl.semaphore_wait(pltpu.get_barrier_semaphore(), 2)
            for n in range(no + 1):
                if n < no:
                    weights[wo_at + 2 * n].wait()
                    far_block(n)
                    first_far(n).start()
                if n > 0:
                    first_far(n - 1).wait()
                    add_up(slice((n - 1) * WIDE, n * WIDE))
                    first_sum(n - 1).start()
                if n < no:
                    weights[wo_at + 2 * n + 1].wait()
                    near_block(n)
            return
        pl.semaphore_wait(free, 1)
        for n in range(no):
            far_block(n)
        far_copy(rows).start()
        for n in range(no):
            near_block(n)
        far_copy(rows).wait()
        add_up(slice(0, half))

    x_copy(0, SMALL).start()
    for s in small:
        s.start()
    for w in weights[: q_at + 1]:
        w.start()
    barrier = pltpu.get_barrier_semaphore()
    for other in (sibling, partner):
        pl.semaphore_signal(barrier, inc=1, device_id=other, device_id_type=MESH)
    for i in range(kv):
        v_s[i, HEAD:, :] = jnp.ones((v_s.shape[1] - HEAD, v_s.shape[2]), v_s.dtype)

    def more():
        pl.semaphore_signal(free, inc=1, device_id=sibling, device_id_type=MESH)

    chunk(0, SMALL, first=True, after_norm=lambda: None)
    more()

    @pl.loop(1, FRONT)
    def _(c):
        o = c * SMALL

        def after_norm():
            @pl.when(c < FRONT - 1)
            def _():
                x_copy(o + SMALL, SMALL).start()

            @pl.when(c == FRONT - 1)
            def _():
                x_copy(o + SMALL, ROWS).start()

        chunk(o, SMALL, after_norm=after_norm)
        peer_copy(c, o, SMALL).start()
        more()

    @pl.loop(FRONT, edge + 1)
    def _(c):
        o = place(c)

        @pl.when(c >= FRONT + LAG)
        def _():
            res_copy(place(c - LAG), ROWS).start()

        def after_norm():
            @pl.when(c < edge)
            def _():
                x_copy(o + ROWS, ROWS).start()

            @pl.when(c == edge)
            def _():
                x_copy(o + ROWS, SMALL).start()

        chunk(o, ROWS, after_norm=after_norm)
        more()

        @pl.when(c < edge)
        def _():
            peer_copy(c, o, ROWS).start()

        @pl.when(c == edge)
        def _():
            edge_copy().start()
            for copy in spread(edge, place(edge), ROWS):
                copy.start()

        @pl.when(c >= FRONT + LAG)
        def _():
            finish(c - LAG, place(c - LAG), ROWS)

    res_copy(place(edge - 1), ROWS).start()

    @pl.loop(0, LATE)
    def _(n):
        o = place(edge + 1) + n * SMALL

        def after_norm():
            @pl.when(n < LATE - 1)
            def _():
                x_copy(o + SMALL, SMALL).start()

        chunk(o, SMALL, after_norm=after_norm)
        for m in range(LATE):

            @pl.when(n == m)
            def _():
                c = edge + 1 + m
                for copy in spread(c, *shape(c)):
                    copy.start()
                late_copy(m, *shape(c)).start()
                if m < LATE - 1:
                    more()

    finish(edge - 1, *shape(edge - 1))
    res_copy(*shape(0)).start()
    finish(0, *shape(0))

    @pl.loop(1, FRONT)
    def _(f):
        res_copy(f * SMALL, SMALL).start()
        finish(f, f * SMALL, SMALL)

    for f in range(last + 1):
        for copy in spread(f, *shape(f)):
            copy.wait()
        if f > edge:
            late_copy(f - edge - 1, *shape(f)).wait()
    edge_copy().wait()


def _copied(done, y, buf, in_sem, out_sem):
    steps, rows = buf.shape[:2]
    here = lambda n: pl.ds(n * rows, rows)
    reads = [pltpu.make_async_copy(done.at[here(n), :], buf.at[n], in_sem.at[n]) for n in range(steps)]
    writes = [pltpu.make_async_copy(buf.at[n], y.at[here(n), :], out_sem.at[n]) for n in range(steps)]
    for copy in reads:
        copy.start()
    for read, write in zip(reads, writes):
        read.wait()
        write.start()
    for copy in writes:
        copy.wait()


def _closed(x, sums, own, other, old, y):
    first = lax.rem(lax.axis_index("tp"), 2) == 0
    half = own.shape[1]
    here = pl.ds(pl.multiple_of(pl.program_id(0) * y.shape[0], y.shape[0]), y.shape[0])
    for n in range(2):
        cols = slice(n * half, (n + 1) * half)
        mine = first if n == 0 else jnp.logical_not(first)

        def add(ref):
            term = sums[here, cols].astype(jnp.float32) + ref[here, :].astype(jnp.float32)
            y[:, cols] = (x[here, cols].astype(jnp.float32) + term).astype(y.dtype)

        pl.when(mine)(lambda: add(own))
        pl.when(jnp.logical_not(mine))(lambda: add(other))


def solution(mesh):
    def layer(x, gain, wq, wk, wv, wo):
        rows, d = x.shape
        chunks = (rows - (FRONT + LATE) * SMALL) // ROWS + FRONT + LATE
        kv = wk.shape[1] // HEAD
        heads = wq.shape[1] // HEAD
        cols = heads // kv * ROWS
        half = d // 2
        bf, f32 = jnp.bfloat16, jnp.float32
        tables = _tables(rows)
        n_weights = 2 + wq.shape[1] // WIDE + d // WIDE
        dma = pltpu.SemaphoreType.DMA
        hbm = pl.BlockSpec(memory_space=pl.ANY)
        sizes = [ROWS] + [SMALL] * LATE
        done = rows - sum(sizes)
        out, crossed, *more = pl.pallas_call(
            _layer,
            out_shape=[
                jax.ShapeDtypeStruct((done, d), bf),
                jax.ShapeDtypeStruct((ROWS, half), bf),
                *[jax.ShapeDtypeStruct((n, d), bf) for n in sizes],
                *[jax.ShapeDtypeStruct((n, half), bf) for n in sizes[1:]],
            ],
            in_specs=[hbm] * 10,
            out_specs=[hbm] * (3 + 2 * LATE),
            scratch_shapes=[
                pltpu.VMEM(gain.shape, bf),
                *[pltpu.VMEM(t.shape, f32) for t in tables],
                pltpu.VMEM(wq.shape, bf),
                pltpu.VMEM((d, 2 * kv * HEAD), bf),
                pltpu.VMEM((wo.shape[0], half), bf),
                pltpu.VMEM((wo.shape[0], half), bf),
                pltpu.VMEM((ROWS, d), bf),
                pltpu.VMEM((ROWS, d), bf),
                pltpu.VMEM((ROWS, half), bf),
                pltpu.VMEM((kv, cols, HEAD), bf),
                pltpu.VMEM((kv, rows, HEAD), bf),
                pltpu.VMEM((kv, HEAD + 16, rows), bf),
                pltpu.VMEM((kv, cols), f32),
                pltpu.VMEM((max(kv * (HEAD + 16), ROWS), max(cols, half)), f32),
                pltpu.VMEM((ROWS, heads * HEAD), bf),
                pltpu.VMEM((ROWS, half), bf),
                pltpu.VMEM((ROWS, half), bf),
                pltpu.VMEM((rows, half), bf),
                pltpu.VMEM((done, half), bf),
                dma((n_weights,)),
                dma((5,)),
                dma,
                dma,
                dma,
                dma,
                pltpu.SemaphoreType.REGULAR,
                dma((chunks,)),
                dma((chunks,)),
                dma((chunks,)),
                dma((chunks,)),
                dma((chunks,)),
                dma((LATE,)),
                dma((2, half // WIDE)),
                dma((2, half // WIDE)),
            ],
            compiler_params=pltpu.CompilerParams(collective_id=0, has_side_effects=True, vmem_limit_bytes=VMEM),
        )(x, gain, *tables, wq, wk, wv, wo)

        def across(a):
            return lax.ppermute(a, "tp", [(i, (i + 2) % 4) for i in range(4)])

        def beside(a):
            return lax.ppermute(a, "tp", [(i, i ^ 1) for i in range(4)])

        sums, late = more[: LATE + 1], more[LATE + 1 :]
        arrived = [crossed]
        for n, a in enumerate(late):
            arrived.append(across(a))

        y = pl.pallas_call(
            _copied,
            out_shape=jax.ShapeDtypeStruct((rows, d), bf),
            in_specs=[hbm],
            out_specs=hbm,
            scratch_shapes=[pltpu.VMEM((done // SMALL, SMALL, d), bf), dma((done // SMALL,)), dma((done // SMALL,))],
            cost_estimate=pl.CostEstimate(flops=10**10, bytes_accessed=4 * done * d, transcendentals=0),
            compiler_params=pltpu.CompilerParams(vmem_limit_bytes=24 * 2**20),
        )(out)
        start = done
        vmem = pl.BlockSpec(memory_space=pltpu.VMEM)
        for own, term in zip(arrived, sums):
            n = own.shape[0]
            if start > done:
                own, y = lax.optimization_barrier((own, y))
            rows_x = lax.slice_in_dim(x, start, start + n)
            other = beside(own)
            y = pl.pallas_call(
                _closed,
                out_shape=jax.ShapeDtypeStruct((rows, d), bf),
                grid=(n // CLOSE,),
                in_specs=[vmem] * 4 + [hbm],
                out_specs=pl.BlockSpec((CLOSE, d), lambda i, at=start // CLOSE: (at + i, 0)),
                input_output_aliases={4: 0},
                cost_estimate=pl.CostEstimate(flops=10**9, bytes_accessed=8 * n * d, transcendentals=0),
                compiler_params=pltpu.CompilerParams(vmem_limit_bytes=24 * 2**20),
            )(rows_x, term, own, other, y)
            start += n
        return y

    tokens, columns = P("dp", None), P(None, "tp")
    return jax.shard_map(
        layer,
        mesh=mesh,
        in_specs=(tokens, P(None), columns, columns, columns, P("tp", None)),
        out_specs=tokens,
        check_vma=False,
    )
```

```python
import jax
import jax.numpy as jnp
import numpy as np
from jax import lax
from jax.experimental import pallas as pl
from jax.experimental.pallas import tpu as pltpu
from jax.sharding import PartitionSpec as P


HEAD = 128
THETA = 10000
LOG2E = 1.4426950408889634
HIDDEN = -2e30
SMALL = 128
FRONT = 4
ROWS = 256
WIDE = 512
STRIP = 512
LAG = 2
CLOSE = 64
LATE = 2
MESH = pl.DeviceIdType.MESH
VMEM = 67_043_328


def _dot(a, b, ca, cb):
    return lax.dot_general(a, b, (((ca,), (cb,)), ((), ())), preferred_element_type=jnp.float32)


def _tables(rows):
    half = HEAD // 2
    rate = THETA ** (-np.arange(half, dtype=np.float64) / half)
    rate = np.concatenate([rate, rate])
    a = np.arange(ROWS)[:, None] * rate
    b = (np.arange(rows // SMALL) * SMALL)[:, None] * rate
    return [t.astype(np.float32) for t in (np.cos(a), np.sin(a), np.cos(b), np.sin(b))]


def _layer(x, gain, cos_a, sin_a, cos_b, sin_b, wq, wk, wv, wo, out, crossed, *rest):
    sums, late, rest = rest[: LATE + 1], rest[LATE + 1 : 2 * LATE + 1], rest[2 * LATE + 1 :]
    _run(x, gain, cos_a, sin_a, cos_b, sin_b, wq, wk, wv, wo, out, sums, crossed, late, *rest)


def _run(x, gain, cos_a, sin_a, cos_b, sin_b, wq, wk, wv, wo, out, sums, crossed, late,
         gain_s, cos_a_s, sin_a_s, cos_b_s, sin_b_s, wq_s, wkv_s, wo_far, wo_near, x_s, a_s, res_s, q_s, k_s, v_s, top_s, wide_s, seen_s,
         far_s, got_s, sum_s, peer_s,
         w_sem, in_sem, x_sem, res_sem, far_send, far_recv, free, sum_send, sum_recv, put_sem, give_send, give_recv, late_sem, first_send, first_recv):
    t = lax.axis_index("tp")
    core = lax.rem(t, 2)
    sibling = {"tp": t + 1 - 2 * core}
    partner = {"tp": lax.rem(t + 2, 4)}
    total_rows, d = x.shape
    edge = (total_rows - (FRONT + LATE) * SMALL) // ROWS + FRONT - 1
    last = edge + LATE
    half = d // 2
    kv = k_s.shape[0]
    heads = wq.shape[1] // HEAD
    group = heads // kv
    near_cols = pl.ds(pl.multiple_of(core * half, half), half)
    nq, nk, no = wq.shape[1] // WIDE, wk.shape[1], half // WIDE
    e = HEAD**-0.5 * LOG2E

    def place(c):
        return FRONT * SMALL + (c - FRONT) * ROWS

    def shape(c):
        if FRONT <= c <= edge:
            return place(c), ROWS
        return (c * SMALL if c < FRONT else place(edge + 1) + (c - edge - 1) * SMALL), SMALL

    def span(o, rows):
        return pl.ds(o if isinstance(o, int) else pl.multiple_of(o, SMALL), rows)

    def block_cols(side, n):
        return pl.ds(pl.multiple_of(side * half + n * WIDE, WIDE), WIDE)

    def static_cols(n):
        return pl.ds(n * WIDE, WIDE)

    weights = [(wk, wkv_s.at[:, pl.ds(0, nk)]), (wv, wkv_s.at[:, pl.ds(nk, nk)])]
    weights += [(wq.at[:, static_cols(n)], wq_s.at[:, static_cols(n)]) for n in range(nq)]
    for n in range(no):
        weights += [(wo.at[:, block_cols(1 - core, n)], wo_far.at[:, static_cols(n)])]
        weights += [(wo.at[:, block_cols(core, n)], wo_near.at[:, static_cols(n)])]
    weights = [pltpu.make_async_copy(src, dst, w_sem.at[n]) for n, (src, dst) in enumerate(weights)]
    q_at, wo_at = 2, 2 + nq
    small = [(gain, gain_s), (cos_a, cos_a_s), (sin_a, sin_a_s), (cos_b, cos_b_s), (sin_b, sin_b_s)]
    small = [pltpu.make_async_copy(src, dst, in_sem.at[n]) for n, (src, dst) in enumerate(small)]

    def x_copy(o, rows):
        return pltpu.make_async_copy(x.at[span(o, rows), :], x_s.at[pl.ds(0, rows), :], x_sem)

    def res_copy(o, rows):
        return pltpu.make_async_copy(x.at[span(o, rows), near_cols], res_s.at[pl.ds(0, rows), :], res_sem)

    def far_copy(rows):
        at = pl.ds(0, rows)
        return pltpu.make_async_remote_copy(src_ref=far_s.at[at, :], dst_ref=got_s.at[at, :], send_sem=far_send, recv_sem=far_recv,
                                            device_id=sibling, device_id_type=MESH)

    def first_far(n):
        there = (pl.ds(0, SMALL), static_cols(n))
        return pltpu.make_async_remote_copy(src_ref=far_s.at[there], dst_ref=got_s.at[there], send_sem=first_send.at[0, n],
                                            recv_sem=first_recv.at[0, n], device_id=sibling, device_id_type=MESH)

    def first_sum(n):
        there = (pl.ds(0, SMALL), static_cols(n))
        return pltpu.make_async_remote_copy(src_ref=sum_s.at[there], dst_ref=peer_s.at[there], send_sem=first_send.at[1, n],
                                            recv_sem=first_recv.at[1, n], device_id=partner, device_id_type=MESH)

    def sum_copy(c, o, rows, target):
        return pltpu.make_async_remote_copy(src_ref=sum_s.at[span(o, rows), :], dst_ref=target, send_sem=sum_send.at[c],
                                            recv_sem=sum_recv.at[c], device_id=partner, device_id_type=MESH)

    def peer_copy(c, o, rows):
        return sum_copy(c, o, rows, peer_s.at[span(o, rows), :])

    def edge_copy():
        return sum_copy(edge, place(edge), ROWS, crossed)

    def put_copy(c, o, rows, target):
        return pltpu.make_async_copy(sum_s.at[span(o, rows), :], target, put_sem.at[c])

    def give_copy(c, o, rows, target):
        return pltpu.make_async_remote_copy(src_ref=sum_s.at[span(o, rows), :], dst_ref=target, send_sem=give_send.at[c],
                                            recv_sem=give_recv.at[c], device_id=sibling, device_id_type=MESH)

    def spread(c, o, rows):
        done = not isinstance(c, int) or c < edge
        target = out.at[span(o, rows), near_cols] if done else sums[c - edge].at[:, near_cols]
        return put_copy(c, o, rows, target), give_copy(c, o, rows, target)

    def late_copy(n, o, rows):
        return pltpu.make_async_copy(sum_s.at[span(o, rows), :], late[n], late_sem.at[n])

    def by_rows(rows, unroll, body):
        @pl.loop(0, rows // 16, unroll=unroll)
        def _(r):
            body(pl.multiple_of(r * 16, 16))

    def finish(c, o, rows):
        res_copy(o, rows).wait()
        if isinstance(c, int) and c == 0:
            for n in range(no):
                first_sum(n).wait()
        else:
            peer_copy(c, o, rows).wait()

        def add(r):
            here = pl.ds(pl.multiple_of(o + r, 16), 16)
            term = sum_s[here, :].astype(jnp.float32) + peer_s[here, :].astype(jnp.float32)
            sum_s[here, :] = (res_s[pl.ds(r, 16), :].astype(jnp.float32) + term).astype(jnp.bfloat16)

        by_rows(rows, 2, add)
        for copy in spread(c, o, rows):
            copy.start()

    def attend(o, rows):
        cols = group * rows
        strip = max(n for n in range(rows, STRIP + 1, rows) if cols % n == 0)
        pieces = [(i, at) for i in range(kv) for at in range(0, cols, strip)]

        def block(at_key, keys, diagonal):
            here = span(at_key, keys)
            scores = [_dot(k_s[i, here, :], q_s[i, at : at + strip, :], 1, 1) for i, at in pieces]
            if diagonal:
                key = lax.broadcasted_iota(jnp.int32, (keys, strip), 0)
                query = lax.rem(lax.broadcasted_iota(jnp.int32, (keys, strip), 1), rows)
                ok = query >= key
            probs, keeps = [], []
            for (i, at), s in zip(pieces, scores):
                there = pl.ds(at, strip)
                if diagonal:
                    s = jnp.where(ok, s, HIDDEN)
                    top = s.max(axis=0, keepdims=True)
                else:
                    old = top_s[i : i + 1, there]
                    top = jnp.maximum(old, s.max(axis=0, keepdims=True))
                    keeps.append(jnp.exp2((old - top) * e))
                top_s[i : i + 1, there] = top
                probs.append(jnp.exp2((s - top) * e).astype(jnp.bfloat16))
            for n, ((i, at), p) in enumerate(zip(pieces, probs)):
                there = pl.ds(at, strip)
                new = _dot(v_s[i, :, here], p, 1, 0)
                deep = pl.ds(i * (HEAD + 16), HEAD + 16)
                wide_s[deep, there] = new if diagonal else wide_s[deep, there] * keeps[n] + new

        block(o, rows, True)
        if isinstance(o, int):
            for k in range(0, o, SMALL):
                block(k, SMALL, False)
        else:

            @pl.loop(0, lax.div(o, ROWS))
            def _(j):
                block(j * ROWS, ROWS, False)

            if rows < ROWS:

                @pl.when(lax.rem(o, ROWS) > 0)
                def _():
                    block(o - SMALL, SMALL, False)

        for i in range(kv):
            for n in range(group):
                there = pl.ds(n * rows, rows)
                h = i * group + n
                top = i * (HEAD + 16)
                done = wide_s[top : top + HEAD, there] * (1 / wide_s[top + HEAD : top + HEAD + 1, there])
                seen_s[pl.ds(0, rows), h * HEAD : (h + 1) * HEAD] = done.T.astype(jnp.bfloat16)

    def chunk(o, rows, first=False, after_norm=None):
        at = pl.ds(0, rows)
        x_copy(o, rows).wait()
        if first:
            for n in range(1, nq):
                weights[q_at + n].start()
            for s in small:
                s.wait()

        def norm(r):
            wide = x_s[pl.ds(r, 16), :].astype(jnp.float32)
            scale = lax.rsqrt(jnp.mean(wide * wide, -1, keepdims=True) + 1e-6)
            a_s[pl.ds(r, 16), :] = (wide * scale * gain_s[...].astype(jnp.float32)).astype(jnp.bfloat16)

        by_rows(rows, 4, norm)
        after_norm()

        sign = jnp.where(lax.broadcasted_iota(jnp.int32, (rows, HEAD), 1) < HEAD // 2, -1.0, 1.0)
        ca, sa = cos_a_s[at, :], sin_a_s[at, :]
        cb, sb = (ref[pl.ds(o // SMALL if isinstance(o, int) else lax.div(o, SMALL), 1), :] for ref in (cos_b_s, sin_b_s))
        cos = ca * cb - sa * sb
        sin = (sa * cb + ca * sb) * sign

        def turned(u):
            u = u.astype(jnp.float32)
            return (u * cos + pltpu.roll(u, HEAD // 2, 1) * sin).astype(jnp.bfloat16)

        if first:
            weights[0].wait()
            weights[1].wait()
        both = _dot(a_s[at, :], wkv_s[...], 1, 0).astype(jnp.bfloat16)
        for i in range(kv):
            k_s[i, span(o, rows), :] = turned(both[:, i * HEAD : (i + 1) * HEAD])
            v_s[i, :HEAD, span(o, rows)] = both[:, nk + i * HEAD : nk + (i + 1) * HEAD].T
        for n in range(nq):
            if first:
                weights[q_at + n].wait()
                for w in weights[wo_at + 2 * n : wo_at + 2 * n + 2]:
                    w.start()
            part = _dot(a_s[at, :], wq_s[:, n * WIDE : (n + 1) * WIDE], 1, 0).astype(jnp.bfloat16)
            for m in range(WIDE // HEAD):
                h = n * (WIDE // HEAD) + m
                q_s[h // group, pl.ds((h % group) * rows, rows), :] = turned(part[:, m * HEAD : (m + 1) * HEAD])

        if first:
            for w in weights[wo_at + 2 * nq :]:
                w.start()
            x_copy(SMALL, SMALL).start()
        attend(o, rows)

        def far_block(n):
            cols = slice(n * WIDE, (n + 1) * WIDE)
            far_s[at, cols] = _dot(seen_s[at, :], wo_far[:, cols], 1, 0).astype(jnp.bfloat16)

        def near_block(n):
            cols = slice(n * WIDE, (n + 1) * WIDE)
            wide_s[at, cols] = _dot(seen_s[at, :], wo_near[:, cols], 1, 0)

        def add_up(cols):
            def add(r):
                near = wide_s[pl.ds(r, 16), cols] + got_s[pl.ds(r, 16), cols].astype(jnp.float32)
                sum_s[pl.ds(pl.multiple_of(o + r, 16), 16), cols] = near.astype(jnp.bfloat16)

            by_rows(rows, 2, add)

        if first:
            pl.semaphore_wait(pltpu.get_barrier_semaphore(), 2)
            for n in range(no + 1):
                if n < no:
                    weights[wo_at + 2 * n].wait()
                    far_block(n)
                    first_far(n).start()
                if n > 0:
                    first_far(n - 1).wait()
                    add_up(slice((n - 1) * WIDE, n * WIDE))
                    first_sum(n - 1).start()
                if n < no:
                    weights[wo_at + 2 * n + 1].wait()
                    near_block(n)
            return
        pl.semaphore_wait(free, 1)
        for n in range(no):
            far_block(n)
        far_copy(rows).start()
        for n in range(no):
            near_block(n)
        far_copy(rows).wait()
        add_up(slice(0, half))

    x_copy(0, SMALL).start()
    for s in small:
        s.start()
    for w in weights[: q_at + 1]:
        w.start()
    barrier = pltpu.get_barrier_semaphore()
    for other in (sibling, partner):
        pl.semaphore_signal(barrier, inc=1, device_id=other, device_id_type=MESH)
    for i in range(kv):
        v_s[i, HEAD:, :] = jnp.ones((v_s.shape[1] - HEAD, v_s.shape[2]), v_s.dtype)

    def more():
        pl.semaphore_signal(free, inc=1, device_id=sibling, device_id_type=MESH)

    chunk(0, SMALL, first=True, after_norm=lambda: None)
    more()

    @pl.loop(1, FRONT)
    def _(c):
        o = c * SMALL

        def after_norm():
            @pl.when(c < FRONT - 1)
            def _():
                x_copy(o + SMALL, SMALL).start()

            @pl.when(c == FRONT - 1)
            def _():
                x_copy(o + SMALL, ROWS).start()

        chunk(o, SMALL, after_norm=after_norm)
        peer_copy(c, o, SMALL).start()
        more()

    @pl.loop(FRONT, edge + 1)
    def _(c):
        o = place(c)

        @pl.when(c >= FRONT + LAG)
        def _():
            res_copy(place(c - LAG), ROWS).start()

        def after_norm():
            @pl.when(c < edge)
            def _():
                x_copy(o + ROWS, ROWS).start()

            @pl.when(c == edge)
            def _():
                x_copy(o + ROWS, SMALL).start()

        chunk(o, ROWS, after_norm=after_norm)
        more()

        @pl.when(c < edge)
        def _():
            peer_copy(c, o, ROWS).start()

        @pl.when((c == edge) & (core == 1))
        def _():
            edge_copy().start()

        @pl.when(c == edge)
        def _():
            for copy in spread(edge, place(edge), ROWS):
                copy.start()

        @pl.when(c >= FRONT + LAG)
        def _():
            finish(c - LAG, place(c - LAG), ROWS)

    res_copy(place(edge - 1), ROWS).start()

    @pl.loop(0, LATE)
    def _(n):
        o = place(edge + 1) + n * SMALL

        def after_norm():
            @pl.when(n < LATE - 1)
            def _():
                x_copy(o + SMALL, SMALL).start()

        chunk(o, SMALL, after_norm=after_norm)
        for m in range(LATE):

            @pl.when(n == m)
            def _():
                c = edge + 1 + m
                for copy in spread(c, *shape(c)):
                    copy.start()
                late_copy(m, *shape(c)).start()
                if m < LATE - 1:
                    more()

    @pl.when(core == 0)
    def _():
        edge_copy().start()

    finish(edge - 1, *shape(edge - 1))
    res_copy(*shape(0)).start()
    finish(0, *shape(0))

    @pl.loop(1, FRONT)
    def _(f):
        res_copy(f * SMALL, SMALL).start()
        finish(f, f * SMALL, SMALL)

    for f in range(last + 1):
        for copy in spread(f, *shape(f)):
            copy.wait()
        if f > edge:
            late_copy(f - edge - 1, *shape(f)).wait()
    edge_copy().wait()


def _copied(done, y, buf, in_sem, out_sem):
    steps, rows = buf.shape[:2]
    here = lambda n: pl.ds(n * rows, rows)
    reads = [pltpu.make_async_copy(done.at[here(n), :], buf.at[n], in_sem.at[n]) for n in range(steps)]
    writes = [pltpu.make_async_copy(buf.at[n], y.at[here(n), :], out_sem.at[n]) for n in range(steps)]
    for copy in reads:
        copy.start()
    for read, write in zip(reads, writes):
        read.wait()
        write.start()
    for copy in writes:
        copy.wait()


def _closed(x, sums, own, other, old, y):
    first = lax.rem(lax.axis_index("tp"), 2) == 0
    half = own.shape[1]
    here = pl.ds(pl.multiple_of(pl.program_id(0) * y.shape[0], y.shape[0]), y.shape[0])
    for n in range(2):
        cols = slice(n * half, (n + 1) * half)
        mine = first if n == 0 else jnp.logical_not(first)

        def add(ref):
            term = sums[here, cols].astype(jnp.float32) + ref[here, :].astype(jnp.float32)
            y[:, cols] = (x[here, cols].astype(jnp.float32) + term).astype(y.dtype)

        pl.when(mine)(lambda: add(own))
        pl.when(jnp.logical_not(mine))(lambda: add(other))


def solution(mesh):
    def layer(x, gain, wq, wk, wv, wo):
        rows, d = x.shape
        chunks = (rows - (FRONT + LATE) * SMALL) // ROWS + FRONT + LATE
        kv = wk.shape[1] // HEAD
        heads = wq.shape[1] // HEAD
        cols = heads // kv * ROWS
        half = d // 2
        bf, f32 = jnp.bfloat16, jnp.float32
        tables = _tables(rows)
        n_weights = 2 + wq.shape[1] // WIDE + d // WIDE
        dma = pltpu.SemaphoreType.DMA
        hbm = pl.BlockSpec(memory_space=pl.ANY)
        sizes = [ROWS] + [SMALL] * LATE
        done = rows - sum(sizes)
        out, crossed, *more = pl.pallas_call(
            _layer,
            out_shape=[
                jax.ShapeDtypeStruct((done, d), bf),
                jax.ShapeDtypeStruct((ROWS, half), bf),
                *[jax.ShapeDtypeStruct((n, d), bf) for n in sizes],
                *[jax.ShapeDtypeStruct((n, half), bf) for n in sizes[1:]],
            ],
            in_specs=[hbm] * 10,
            out_specs=[hbm] * (3 + 2 * LATE),
            scratch_shapes=[
                pltpu.VMEM(gain.shape, bf),
                *[pltpu.VMEM(t.shape, f32) for t in tables],
                pltpu.VMEM(wq.shape, bf),
                pltpu.VMEM((d, 2 * kv * HEAD), bf),
                pltpu.VMEM((wo.shape[0], half), bf),
                pltpu.VMEM((wo.shape[0], half), bf),
                pltpu.VMEM((ROWS, d), bf),
                pltpu.VMEM((ROWS, d), bf),
                pltpu.VMEM((ROWS, half), bf),
                pltpu.VMEM((kv, cols, HEAD), bf),
                pltpu.VMEM((kv, rows, HEAD), bf),
                pltpu.VMEM((kv, HEAD + 16, rows), bf),
                pltpu.VMEM((kv, cols), f32),
                pltpu.VMEM((max(kv * (HEAD + 16), ROWS), max(cols, half)), f32),
                pltpu.VMEM((ROWS, heads * HEAD), bf),
                pltpu.VMEM((ROWS, half), bf),
                pltpu.VMEM((ROWS, half), bf),
                pltpu.VMEM((rows, half), bf),
                pltpu.VMEM((done, half), bf),
                dma((n_weights,)),
                dma((5,)),
                dma,
                dma,
                dma,
                dma,
                pltpu.SemaphoreType.REGULAR,
                dma((chunks,)),
                dma((chunks,)),
                dma((chunks,)),
                dma((chunks,)),
                dma((chunks,)),
                dma((LATE,)),
                dma((2, half // WIDE)),
                dma((2, half // WIDE)),
            ],
            compiler_params=pltpu.CompilerParams(collective_id=0, has_side_effects=True, vmem_limit_bytes=VMEM),
        )(x, gain, *tables, wq, wk, wv, wo)

        def across(a):
            return lax.ppermute(a, "tp", [(i, (i + 2) % 4) for i in range(4)])

        def beside(a):
            return lax.ppermute(a, "tp", [(i, i ^ 1) for i in range(4)])

        sums, late = more[: LATE + 1], more[LATE + 1 :]
        arrived = [crossed]
        for n, a in enumerate(late):
            arrived.append(across(a))

        y = pl.pallas_call(
            _copied,
            out_shape=jax.ShapeDtypeStruct((rows, d), bf),
            in_specs=[hbm],
            out_specs=hbm,
            scratch_shapes=[pltpu.VMEM((done // SMALL, SMALL, d), bf), dma((done // SMALL,)), dma((done // SMALL,))],
            cost_estimate=pl.CostEstimate(flops=10**10, bytes_accessed=4 * done * d, transcendentals=0),
            compiler_params=pltpu.CompilerParams(vmem_limit_bytes=24 * 2**20),
        )(out)
        start = done
        vmem = pl.BlockSpec(memory_space=pltpu.VMEM)
        for own, term in zip(arrived, sums):
            n = own.shape[0]
            if start > done:
                own, y = lax.optimization_barrier((own, y))
            rows_x = lax.slice_in_dim(x, start, start + n)
            other = beside(own)
            y = pl.pallas_call(
                _closed,
                out_shape=jax.ShapeDtypeStruct((rows, d), bf),
                grid=(n // CLOSE,),
                in_specs=[vmem] * 4 + [hbm],
                out_specs=pl.BlockSpec((CLOSE, d), lambda i, at=start // CLOSE: (at + i, 0)),
                input_output_aliases={4: 0},
                cost_estimate=pl.CostEstimate(flops=10**9, bytes_accessed=8 * n * d, transcendentals=0),
                compiler_params=pltpu.CompilerParams(vmem_limit_bytes=24 * 2**20),
            )(rows_x, term, own, other, y)
            start += n
        return y

    tokens, columns = P("dp", None), P(None, "tp")
    return jax.shard_map(
        layer,
        mesh=mesh,
        in_specs=(tokens, P(None), columns, columns, columns, P("tp", None)),
        out_specs=tokens,
        check_vma=False,
    )
```
